16 devices in a mesh: dp: 4 (over y, z, core), tp: 4 (over x).
Axes of the slice: x: 4, y: 2, z: 1, core: 2. Of those that a mesh axis runs over, the one named last changes fastest.
The devices are a block of a 4x4x8 slice.
Arguments:
- x: bfloat16 [8192, 2048], P('dp'), parts along dimension 0
- dy: bfloat16 [8192, 2048], P('dp'), parts along dimension 0
- gate: bfloat16 [8192, 5120], P('dp', 'tp'), parts along dimension 0
- up: bfloat16 [8192, 5120], P('dp', 'tp'), parts along dimension 0
- w_gate: bfloat16 [2048, 5120], P(None, 'tp')
- w_up: bfloat16 [2048, 5120], P(None, 'tp')
- w_down: bfloat16 [5120, 2048], P('tp')
Outputs:
- output 1: bfloat16 [8192, 2048], P('dp'), parts along dimension 0
- output 2: bfloat16 [8192, 5120], P('dp', 'tp'), parts along dimension 0
- output 3: bfloat16 [8192, 5120], P('dp', 'tp'), parts along dimension 0
- output 4: bfloat16 [20480, 2048], P(('dp', 'tp')), parts along dimension 0
There are 4 independent parts. The reference program is written for one: setup_inputs(seed, part) draws one part's arguments, and reference() takes and returns one part's arrays. A program takes and returns all parts, laid end to end along the dimension named above; an argument that names none is the same for every part.
All inputs are finite; a program needn't handle non-finite values.
Results may differ from the reference program's by a relative error of at most 0.012.
Values are sent between devices in bfloat16 or wider.
A program may use at most 768 MiB of HBM per device.

```python
import jax
import jax.numpy as jnp

ROWS = 2048
D = 2048
FF = 5120


def act(gate, up):
    return jax.nn.gelu(gate) * up


def setup_inputs(seed: int = 0, part: int = 0) -> dict:
    kx, ky, ka, kb, kg, ku, kd = jax.random.split(jax.random.key(seed), 7)
    kx, ky, ka, kb = (jax.random.fold_in(k, part) for k in (kx, ky, ka, kb))
    drawn = {
        "x": jax.random.normal(kx, (ROWS, D), jnp.float32),
        "dy": jax.random.normal(ky, (ROWS, D), jnp.float32),
        "gate": jax.random.normal(ka, (ROWS, FF), jnp.float32),
        "up": jax.random.normal(kb, (ROWS, FF), jnp.float32),
        "w_gate": jax.random.normal(kg, (D, FF), jnp.float32) * D**-0.5,
        "w_up": jax.random.normal(ku, (D, FF), jnp.float32) * D**-0.5,
        "w_down": jax.random.normal(kd, (FF, D), jnp.float32) * FF**-0.5,
    }
    return {k: v.astype(jnp.bfloat16) for k, v in drawn.items()}


def reference(x, dy, gate, up, w_gate, w_up, w_down):
    hidden, back = jax.vjp(act, gate.astype(jnp.float32), up.astype(jnp.float32))
    d_hidden = jnp.dot(dy, w_down.T, preferred_element_type=jnp.float32)
    d_gate, d_up = (g.astype(jnp.bfloat16) for g in back(d_hidden))
    dx = jnp.dot(d_gate, w_gate.T, preferred_element_type=jnp.float32) + jnp.dot(d_up, w_up.T, preferred_element_type=jnp.float32)
    dw_gate = jnp.dot(x.T, d_gate, preferred_element_type=jnp.float32)
    dw_up = jnp.dot(x.T, d_up, preferred_element_type=jnp.float32)
    dw_down = jnp.dot(hidden.astype(jnp.bfloat16).T, dy, preferred_element_type=jnp.float32)
    return tuple(g.astype(jnp.bfloat16) for g in (dx, dw_gate, dw_up, dw_down))
```

```python
import functools
import math

import jax
import jax.numpy as jnp
from jax import lax
from jax.experimental import pallas as pl
from jax.experimental.pallas import tpu as pltpu
from jax.sharding import PartitionSpec as P

MESH = pl.DeviceIdType.MESH
ANY = pl.BlockSpec(memory_space=pl.ANY)
BF16, F32 = jnp.bfloat16, jnp.float32
C = math.sqrt(2.0 / math.pi)
BLK = 256
NT = 256
XT = 256


def dot(a, b, ca, cb):
    return lax.dot_general(a, b, (((ca,), (cb,)), ((), ())), preferred_element_type=F32)


def ring_kernel(
    x, dy, gate, up, w_gate, w_up, w_down,
    own_a, own_b, r_a, r_b, l_a, l_b, hid, dw_gate, dw_up,
    wg, wu, wd, dg, du, dyb, gb, ub, hidb, snd, rcv, own, xb, og, ou,
    wd_sem, w_sem, blk_sem, hid_sem, ssem, rsem, ag_ssem, ag_rsem, own_sem, x_sem, o_sem,
):
    me = lax.axis_index("tp")
    right, left = lax.rem(me + 1, 4), lax.rem(me + 3, 4)
    rows, width = dy.shape
    ff = gate.shape[1]
    chunk, half = rows // 4, width // 2

    order = ((2, 0), (2, 1), (3, 0), (1, 0), (3, 1), (1, 1), (0, 0), (0, 1))

    def start_row(j):
        k, b = order[j]
        return pl.multiple_of(lax.rem(me + k, 4) * chunk + b * BLK, BLK)

    def block_copies(j):
        s, r = j % 2, pl.ds(start_row(j), BLK)
        return (
            pltpu.make_async_copy(dy.at[r], dyb.at[s], blk_sem.at[s, 0]),
            pltpu.make_async_copy(gate.at[r], gb.at[s], blk_sem.at[s, 1]),
            pltpu.make_async_copy(up.at[r], ub.at[s], blk_sem.at[s, 2]),
        )

    def wd_copy(n):
        r = pl.ds(n * NT, NT)
        return pltpu.make_async_copy(w_down.at[r], wd.at[r], wd_sem.at[n])

    def w_copy(i, h):
        r = pl.ds(h * half, half)
        return pltpu.make_async_copy((w_gate, w_up)[i].at[r], (wg, wu)[i].at[r], w_sem.at[i, h])

    nt = ff // NT
    first = block_copies(0)
    first[0].start()
    wd_copy(0).start()
    first[1].start()
    first[2].start()
    for n in range(1, nt):
        wd_copy(n).start()
    for h in range(2):
        for i in range(2):
            w_copy(i, h).start()
    for c in block_copies(1):
        c.start()

    barrier = pltpu.get_barrier_semaphore()
    for d in (left, right):
        pl.semaphore_signal(barrier, inc=1, device_id={"tp": d}, device_id_type=MESH)

    def hid_copy(j):
        return pltpu.make_async_copy(hidb.at[j % 2], hid.at[pl.ds(start_row(j), BLK)], hid_sem.at[j % 2])

    def hidden(j):
        s, r0 = j % 2, start_row(j)
        for c in block_copies(j):
            c.wait()
        if j >= 2:
            hid_copy(j - 2).wait()

        def tile(n):
            cols = pl.ds(pl.multiple_of(n * NT, NT), NT)
            dh = dot(dyb[s], wd[cols, :], 1, 1)
            g = gb[s, :, cols].astype(F32)
            u = ub[s, :, cols].astype(F32)
            g2 = g * g
            t = jnp.tanh(C * (g + 0.044715 * (g * g2)))
            cdf = 0.5 * (1.0 + t)
            act = g * cdf
            hidb[s, :, cols] = (act * u).astype(BF16)
            du[pl.ds(r0, BLK), cols] = (dh * act).astype(BF16)
            slope = cdf + (0.5 * C) * g * (1.0 - t * t) * (1.0 + (3 * 0.044715) * g2)
            dg[pl.ds(r0, BLK), cols] = (dh * u * slope).astype(BF16)

        if j == 0:
            for n in range(nt):
                wd_copy(n).wait()
                tile(n)
        else:
            pl.loop(0, nt)(tile)
        if j + 2 < len(order):
            for c in block_copies(j + 2):
                c.start()
        hid_copy(j).start()

    def term(j, h, adds, dst, row):
        r = pl.ds(start_row(j), BLK)
        if j == 0:
            w_copy(0, h).wait()
            w_copy(1, h).wait()

        @pl.loop(0, half // 512)
        def _(i):
            wr = pl.ds(pl.multiple_of(h * half + i * 512, 512), 512)
            cols = pl.ds(pl.multiple_of(i * 512, 512), 512)
            t = dot(dg[r, :], wg[wr, :], 1, 1) + dot(du[r, :], wu[wr, :], 1, 1)
            for a in adds:
                t = t + rcv[a, :, cols].astype(F32)
            dst[row : row + BLK, cols] = t.astype(BF16)

    def slot(kind, b):
        return kind * 2 + b

    def reduce_copy(kind, b):
        s = slot(kind, b)
        return pltpu.make_async_remote_copy(
            src_ref=snd.at[s], dst_ref=rcv.at[s], send_sem=ssem.at[s], recv_sem=rsem.at[s],
            device_id={"tp": left if kind < 3 else right}, device_id_type=MESH,
        )

    def send(j, h, kind, adds=()):
        b = order[j][1]
        term(j, h, adds, snd.at[slot(kind, b)], 0)
        reduce_copy(kind, b).start()

    hidden(0)
    term(0, 0, (), snd.at[slot(0, 0)], 0)
    pl.semaphore_wait(barrier, 2)
    reduce_copy(0, 0).start()
    send(0, 1, 3)
    hidden(1)
    send(1, 0, 0)
    send(1, 1, 3)
    for j, h, kind in ((2, 1, 1), (3, 0, 4), (4, 1, 1), (5, 0, 4)):
        hidden(j)
        send(j, h, kind)
    for b in range(2):
        reduce_copy(0, b).wait_recv()
        send(2 + 2 * b, 0, 2, (slot(0, b),))
        reduce_copy(3, b).wait_recv()
        send(3 + 2 * b, 1, 5, (slot(3, b),))
    hidden(6)
    hidden(7)

    steps = width // XT

    def x_copy(i, s):
        return pltpu.make_async_copy(x.at[:, pl.ds(pl.multiple_of(i * XT, XT), XT)], xb.at[s], x_sem.at[s])

    def o_copies(i, s):
        r = pl.ds(pl.multiple_of(i * XT, XT), XT)
        return (
            pltpu.make_async_copy(og.at[s], dw_gate.at[r], o_sem.at[s, 0]),
            pltpu.make_async_copy(ou.at[s], dw_up.at[r], o_sem.at[s, 1]),
        )

    def weights(lo, hi):
        x_copy(lo, 0).start()
        x_copy(lo + 1, 1).start()

        @pl.loop(0, (hi - lo) // 2)
        def _(p):
            for s in range(2):
                i = lo + 2 * p + s
                x_copy(i, s).wait()

                @pl.when(p > 0)
                def _():
                    for c in o_copies(i, s):
                        c.wait()

                og[s] = dot(xb[s], dg[...], 0, 0).astype(BF16)
                ou[s] = dot(xb[s], du[...], 0, 0).astype(BF16)

                @pl.when(i + 2 < hi)
                def _():
                    x_copy(i + 2, s).start()

                for c in o_copies(i, s):
                    c.start()

        for s in range(2):
            for c in o_copies(hi - 2 + s, s):
                c.wait()

    def gather_copies(b):
        r = pl.ds(b * BLK, BLK)
        for d, h, dst in ((left, 0, r_a), (right, 1, l_b), (left, 1, r_b), (right, 0, l_a)):
            i = b * 4 + (0 if d is left else 2) + h
            yield pltpu.make_async_remote_copy(
                src_ref=own.at[h, r], dst_ref=dst.at[r], send_sem=ag_ssem.at[i], recv_sem=ag_rsem.at[i],
                device_id={"tp": d}, device_id_type=MESH,
            )

    def own_copies(b):
        r = pl.ds(b * BLK, BLK)
        return (
            pltpu.make_async_copy(own.at[0, r], own_a.at[r], own_sem.at[b, 0]),
            pltpu.make_async_copy(own.at[1, r], own_b.at[r], own_sem.at[b, 1]),
        )

    def finish(b):
        reduce_copy(4, b).wait_recv()
        reduce_copy(2, b).wait_recv()
        term(6 + b, 0, (slot(2, b), slot(4, b)), own.at[0], b * BLK)
        reduce_copy(1, b).wait_recv()
        reduce_copy(5, b).wait_recv()
        term(6 + b, 1, (slot(5, b), slot(1, b)), own.at[1], b * BLK)
        for c in gather_copies(b):
            c.start()
        for c in own_copies(b):
            c.start()

    weights(0, steps // 2)
    finish(0)
    finish(1)
    weights(steps // 2, steps)

    for kind in range(6):
        for b in range(2):
            reduce_copy(kind, b).wait_send()
    for b in range(2):
        for c in gather_copies(b):
            c.wait()
        for c in own_copies(b):
            c.wait()
    hid_copy(6).wait()
    hid_copy(7).wait()


def ring(x, dy, gate, up, w_gate, w_up, w_down):
    rows, width = dy.shape
    ff = gate.shape[1]
    chunk, half = rows // 4, width // 2
    piece = jax.ShapeDtypeStruct((chunk, half), BF16)
    dma = pltpu.SemaphoreType.DMA
    return pl.pallas_call(
        ring_kernel,
        name="ring",
        out_shape=(piece,) * 6
        + (jax.ShapeDtypeStruct((rows, ff), BF16),)
        + (jax.ShapeDtypeStruct((width, ff), BF16),) * 2,
        in_specs=[ANY] * 7,
        out_specs=(ANY,) * 9,
        scratch_shapes=[
            pltpu.VMEM((width, ff), BF16),
            pltpu.VMEM((width, ff), BF16),
            pltpu.VMEM((ff, width), BF16),
            pltpu.VMEM((rows, ff), BF16),
            pltpu.VMEM((rows, ff), BF16),
            pltpu.VMEM((2, BLK, width), BF16),
            pltpu.VMEM((2, BLK, ff), BF16),
            pltpu.VMEM((2, BLK, ff), BF16),
            pltpu.VMEM((2, BLK, ff), BF16),
            pltpu.VMEM((12, BLK, half), BF16),
            pltpu.VMEM((12, BLK, half), BF16),
            pltpu.VMEM((2, chunk, half), BF16),
            pltpu.VMEM((2, rows, XT), BF16),
            pltpu.VMEM((2, XT, ff), BF16),
            pltpu.VMEM((2, XT, ff), BF16),
            dma((ff // NT,)),
            dma((2, 2)),
            dma((2, 3)),
            dma((2,)),
            dma((12,)),
            dma((12,)),
            dma((8,)),
            dma((8,)),
            dma((2, 2)),
            dma((2,)),
            dma((2, 2)),
        ],
        compiler_params=pltpu.CompilerParams(collective_id=0, has_side_effects=True, vmem_limit_bytes=60 << 20),
        cost_estimate=pl.CostEstimate(flops=10 * rows * width * ff, bytes_accessed=100 << 20, transcendentals=rows * ff),
    )(x, dy, gate, up, w_gate, w_up, w_down)


def place_copies(pairs, stage, sems):
    return [
        (pltpu.make_async_copy(s, v, sems.at[i, 0]), pltpu.make_async_copy(v, d, sems.at[i, 1]))
        for i, ((s, d), v) in enumerate(zip(pairs, stage))
    ]


def rest_kernel(hid, dy, own_a, own_b, r_a, r_b, l_a, l_b, g_in, u_in, dw_down, dx, g_out, u_out, pieces, gu, sems):
    me = lax.axis_index("tp")
    chunk, half = own_a.shape
    step, last = pl.program_id(0), pl.num_programs(0) - 1
    pairs, stage = [(g_in, g_out), (u_in, u_out)], [gu.at[0], gu.at[1]]
    for k, (a, b) in ((0, (own_a, own_b)), (1, (r_a, r_b)), (3, (l_a, l_b))):
        r = pl.ds(pl.multiple_of(lax.rem(me + k, 4) * chunk, chunk), chunk)
        for h, src in enumerate((a, b)):
            stage.append(pieces.at[len(pairs) - 2])
            pairs.append((src, dx.at[r, pl.ds(h * half, half)]))
    copies = place_copies(pairs, stage, sems)

    @pl.when(step == 0)
    def _():
        for read, _ in copies:
            read.start()

    dw_down[...] = dot(hid[...], dy[...], 0, 0).astype(BF16)

    @pl.when(step == 1)
    def _():
        for read, write in copies:
            read.wait()
            write.start()

    @pl.when(step == last)
    def _():
        for _, write in copies:
            write.wait()


def rest(hid, dy, pieces, dw_gate, dw_up):
    rows, width = dy.shape
    ff = hid.shape[1]
    chunk, half = rows // 4, width // 2
    return pl.pallas_call(
        rest_kernel,
        name="rest",
        grid=(ff // NT,),
        out_shape=(
            jax.ShapeDtypeStruct((ff, width), BF16),
            jax.ShapeDtypeStruct((rows, width), BF16),
            jax.ShapeDtypeStruct(dw_gate.shape, BF16),
            jax.ShapeDtypeStruct(dw_up.shape, BF16),
        ),
        in_specs=[pl.BlockSpec((rows, NT), lambda i: (0, i)), pl.BlockSpec((rows, width), lambda i: (0, 0))] + [ANY] * 8,
        out_specs=(pl.BlockSpec((NT, width), lambda i: (i, 0)), ANY, ANY, ANY),
        scratch_shapes=[
            pltpu.VMEM((6, chunk, half), BF16),
            pltpu.VMEM((2,) + dw_gate.shape, BF16),
            pltpu.SemaphoreType.DMA((8, 2)),
        ],
        compiler_params=pltpu.CompilerParams(vmem_limit_bytes=56 << 20),
        cost_estimate=pl.CostEstimate(flops=2 * rows * width * ff, bytes_accessed=60 << 20, transcendentals=0),
    )(hid, dy, *pieces, dw_gate, dw_up)


def place_kernel(p_a, p_b, dx_in, dx, stage, sems):
    me = lax.axis_index("tp")
    chunk, half = p_a.shape
    r = pl.ds(pl.multiple_of(lax.rem(me + 2, 4) * chunk, chunk), chunk)
    pairs = [(src, dx.at[r, pl.ds(h * half, half)]) for h, src in enumerate((p_a, p_b))]
    copies = place_copies(pairs, [stage.at[0], stage.at[1]], sems)
    for read, _ in copies:
        read.start()
    for read, write in copies:
        read.wait()
        write.start()
    for _, write in copies:
        write.wait()


def place(p_a, p_b, dx):
    return pl.pallas_call(
        place_kernel,
        name="place",
        out_shape=jax.ShapeDtypeStruct(dx.shape, dx.dtype),
        in_specs=[ANY] * 3,
        out_specs=ANY,
        scratch_shapes=[pltpu.VMEM((2,) + p_a.shape, BF16), pltpu.SemaphoreType.DMA((2, 2))],
        input_output_aliases={2: 0},
        compiler_params=pltpu.CompilerParams(vmem_limit_bytes=8 << 20),
    )(p_a, p_b, dx)


def solution(mesh):
    n = mesh.shape["tp"]
    assert n == 4
    to_left = [(i, (i - 1) % n) for i in range(n)]
    to_right = [(i, (i + 1) % n) for i in range(n)]

    def step(x, dy, gate, up, w_gate, w_up, w_down):
        *pieces, hid, dw_gate, dw_up = ring(x, dy, gate, up, w_gate, w_up, w_down)
        p_a = lax.ppermute(pieces[2], "tp", to_left)
        p_b = lax.ppermute(pieces[5], "tp", to_right)
        dw_down, dx, dw_gate, dw_up = rest(hid, dy, pieces, dw_gate, dw_up)
        return place(p_a, p_b, dx), dw_gate, dw_up, dw_down

    tokens, columns, rows = P("dp", None), P(None, "tp"), P("tp", None)
    return jax.shard_map(
        step,
        mesh=mesh,
        in_specs=(tokens, tokens, P("dp", "tp"), P("dp", "tp"), columns, columns, rows),
        out_specs=(tokens, P("dp", "tp"), P("dp", "tp"), P(("dp", "tp"), None)),
        check_vma=False,
    )
```

```python
import functools
import math

import jax
import jax.numpy as jnp
from jax import lax
from jax.experimental import pallas as pl
from jax.experimental.pallas import tpu as pltpu
from jax.sharding import PartitionSpec as P

MESH = pl.DeviceIdType.MESH
ANY = pl.BlockSpec(memory_space=pl.ANY)
BF16, F32 = jnp.bfloat16, jnp.float32
C = math.sqrt(2.0 / math.pi)
BLK = 256
NT = 256
DT = 512
AHEAD = 3
XT = 256

ORDER = ((2, 0), (2, 1), (3, 0), (1, 0), (3, 1), (1, 1), (0, 0), (0, 1))


def dot(a, b, ca, cb):
    return lax.dot_general(a, b, (((ca,), (cb,)), ((), ())), preferred_element_type=F32)


def ring_kernel(
    x, dy, gate, up, w_gate, w_up, w_down,
    own_a, own_b, r_a, r_b, l_a, l_b, hid, dw_gate, dw_up,
    wg, wu, wd, dg, du, dyb, gb, ub, hidb, snd, rcv, own, xb, og, ou,
    wd_sem, w_sem, blk_sem, hid_sem, ssem, rsem, head_ssem, head_rsem, ag_ssem, ag_rsem, own_sem, x_sem, o_sem,
):
    me = lax.axis_index("tp")
    right, left = lax.rem(me + 1, 4), lax.rem(me + 3, 4)
    rows, width = dy.shape
    ff = gate.shape[1]
    chunk, half = rows // 4, width // 2

    def start_row(j):
        k, b = ORDER[j]
        return pl.multiple_of(lax.rem(me + k, 4) * chunk + b * BLK, BLK)

    def block_copies(j):
        s, r = j % 2, pl.ds(start_row(j), BLK)
        return [
            pltpu.make_async_copy(dy.at[r], dyb.at[s], blk_sem.at[s, 0]),
            pltpu.make_async_copy(gate.at[r], gb.at[s], blk_sem.at[s, 1]),
            pltpu.make_async_copy(up.at[r], ub.at[s], blk_sem.at[s, 2]),
        ]

    def span(n, size):
        return pl.ds(n * size if isinstance(n, int) else pl.multiple_of(n * size, size), size)

    def wd_copy(n):
        r = span(n, NT)
        return pltpu.make_async_copy(w_down.at[r], wd.at[r], wd_sem.at[n])

    def w_copies(q):
        r = span(q, DT)
        return (
            pltpu.make_async_copy(w_gate.at[r], wg.at[r], w_sem.at[0, q]),
            pltpu.make_async_copy(w_up.at[r], wu.at[r], w_sem.at[1, q]),
        )

    def start(copies):
        for c in copies:
            c.start()

    nt, per_half = ff // NT, half // DT
    first = block_copies(0)
    start(first[:1] + [wd_copy(0)] + first[1:] + [wd_copy(n) for n in range(1, AHEAD)])

    barrier = pltpu.get_barrier_semaphore()
    for d in (left, right):
        pl.semaphore_signal(barrier, inc=1, device_id={"tp": d}, device_id_type=MESH)

    def hid_copy(j):
        return pltpu.make_async_copy(hidb.at[j % 2], hid.at[pl.ds(start_row(j), BLK)], hid_sem.at[j % 2])

    def backward(j, n, dh):
        s, r, cols = j % 2, pl.ds(start_row(j), BLK), span(n, NT)
        g = gb[s, :, cols].astype(F32)
        u = ub[s, :, cols].astype(F32)
        g2 = g * g
        t = jnp.tanh(C * (g + 0.044715 * (g * g2)))
        cdf = 0.5 * (1.0 + t)
        act = g * cdf
        hidb[s, :, cols] = (act * u).astype(BF16)
        du[r, cols] = (dh * act).astype(BF16)
        slope = cdf + (0.5 * C) * g * (1.0 - t * t) * (1.0 + (3 * 0.044715) * g2)
        dg[r, cols] = (dh * u * slope).astype(BF16)

    def hidden_first():
        for c in first:
            c.wait()

        @pl.loop(0, nt)
        def _(n):
            wd_copy(n).wait()

            @pl.when(n < nt - AHEAD)
            def _():
                wd_copy(n + AHEAD).start()

            @pl.when(n >= nt - AHEAD)
            def _():
                i = n - (nt - AHEAD)
                start(w_copies(lax.rem(i, 2) * per_half + i // 2))

            backward(0, n, dot(dyb[0], wd[span(n, NT), :], 1, 1))

        for i in range(AHEAD, 2 * per_half):
            start(w_copies(i % 2 * per_half + i // 2))
        start(block_copies(1))
        hid_copy(0).start()

    def hidden(j):
        s = j % 2
        for c in block_copies(j):
            c.wait()
        if j >= 2:
            hid_copy(j - 2).wait()

        @pl.loop(0, nt)
        def _(n):
            backward(j, n, dot(dyb[s], wd[span(n, NT), :], 1, 1))

        if j < len(ORDER) - 2:
            for c in block_copies(j + 2):
                c.start()
        hid_copy(j).start()

    def columns(j, q, adds, dst, rows_, cols):
        r, wr = pl.ds(start_row(j), BLK), span(q, DT)
        t = dot(dg[r, :], wg[wr, :], 1, 1) + dot(du[r, :], wu[wr, :], 1, 1)
        for a in adds:
            t = t + rcv[a, :, cols].astype(F32)
        dst[rows_, cols] = t.astype(BF16)

    def term(j, h, adds, dst, row):
        @pl.loop(0, per_half)
        def _(i):
            columns(j, h * per_half + i, adds, dst, pl.ds(row, BLK), span(i, DT))

    def slot(kind, b):
        return kind * 2 + b

    def reduce_copy(kind, b, rect=None):
        s = slot(kind, b)
        src, dst, sems = snd.at[s], rcv.at[s], (ssem.at[s], rsem.at[s])
        if rect is not None:
            src, dst = src.at[:, span(rect, DT)], dst.at[:, span(rect, DT)]
            sems = (head_ssem.at[kind // 3, rect], head_rsem.at[kind // 3, rect])
        return pltpu.make_async_remote_copy(
            src_ref=src, dst_ref=dst, send_sem=sems[0], recv_sem=sems[1],
            device_id={"tp": left if kind < 3 else right}, device_id_type=MESH,
        )

    def send(j, h, kind, adds=()):
        b = ORDER[j][1]
        term(j, h, adds, snd.at[slot(kind, b)], 0)
        reduce_copy(kind, b).start()

    head = range(per_half)
    hidden_first()
    pl.semaphore_wait(barrier, 2)

    @pl.loop(0, per_half)
    def _(i):
        for h, kind in ((0, 0), (1, 3)):
            q = h * per_half + i
            for c in w_copies(q):
                c.wait()
            columns(0, q, (), snd.at[slot(kind, 0)], pl.ds(0, BLK), span(i, DT))
            reduce_copy(kind, 0, i).start()

    start(block_copies(2))
    hidden(1)
    send(1, 0, 0)
    send(1, 1, 3)
    for j, h, kind in ((2, 1, 1), (3, 0, 4), (4, 1, 1), (5, 0, 4)):
        hidden(j)
        send(j, h, kind)
    for b in range(2):
        for kind, j, h in ((0, 2, 0), (3, 3, 1)):
            for i in head if b == 0 else (None,):
                reduce_copy(kind, b, i).wait_recv()
            send(j + 2 * b, h, kind + 2, (slot(kind, b),))
    hidden(6)
    hidden(7)

    steps = width // XT

    def x_copy(i, s):
        return pltpu.make_async_copy(x.at[:, pl.ds(pl.multiple_of(i * XT, XT), XT)], xb.at[s], x_sem.at[s])

    def o_copies(i, s):
        r = pl.ds(pl.multiple_of(i * XT, XT), XT)
        return (
            pltpu.make_async_copy(og.at[s], dw_gate.at[r], o_sem.at[s, 0]),
            pltpu.make_async_copy(ou.at[s], dw_up.at[r], o_sem.at[s, 1]),
        )

    def weights(lo, hi):
        x_copy(lo, 0).start()
        x_copy(lo + 1, 1).start()

        @pl.loop(0, (hi - lo) // 2)
        def _(p):
            for s in range(2):
                i = lo + 2 * p + s
                x_copy(i, s).wait()

                @pl.when(p > 0)
                def _():
                    for c in o_copies(i, s):
                        c.wait()

                og[s] = dot(xb[s], dg[...], 0, 0).astype(BF16)
                ou[s] = dot(xb[s], du[...], 0, 0).astype(BF16)

                @pl.when(i + 2 < hi)
                def _():
                    x_copy(i + 2, s).start()

                for c in o_copies(i, s):
                    c.start()

        for s in range(2):
            for c in o_copies(hi - 2 + s, s):
                c.wait()

    def gather_copies(b):
        r = pl.ds(b * BLK, BLK)
        for d, h, dst in ((left, 0, r_a), (right, 1, l_b), (left, 1, r_b), (right, 0, l_a)):
            i = b * 4 + (0 if d is left else 2) + h
            yield pltpu.make_async_remote_copy(
                src_ref=own.at[h, r], dst_ref=dst.at[r], send_sem=ag_ssem.at[i], recv_sem=ag_rsem.at[i],
                device_id={"tp": d}, device_id_type=MESH,
            )

    def own_copies(b):
        r = pl.ds(b * BLK, BLK)
        return (
            pltpu.make_async_copy(own.at[0, r], own_a.at[r], own_sem.at[b, 0]),
            pltpu.make_async_copy(own.at[1, r], own_b.at[r], own_sem.at[b, 1]),
        )

    def finish(b):
        reduce_copy(4, b).wait_recv()
        reduce_copy(2, b).wait_recv()
        term(6 + b, 0, (slot(2, b), slot(4, b)), own.at[0], b * BLK)
        reduce_copy(1, b).wait_recv()
        reduce_copy(5, b).wait_recv()
        term(6 + b, 1, (slot(5, b), slot(1, b)), own.at[1], b * BLK)
        for c in gather_copies(b):
            c.start()
        for c in own_copies(b):
            c.start()

    weights(0, steps // 2)
    finish(0)
    finish(1)
    weights(steps // 2, steps)

    for kind in range(6):
        for b in range(2):
            for i in head if kind % 3 == 0 and b == 0 else (None,):
                reduce_copy(kind, b, i).wait_send()
    for b in range(2):
        for c in gather_copies(b):
            c.wait()
        for c in own_copies(b):
            c.wait()
    hid_copy(6).wait()
    hid_copy(7).wait()


def ring(x, dy, gate, up, w_gate, w_up, w_down):
    rows, width = dy.shape
    ff = gate.shape[1]
    chunk, half = rows // 4, width // 2
    piece = jax.ShapeDtypeStruct((chunk, half), BF16)
    dma = pltpu.SemaphoreType.DMA
    return pl.pallas_call(
        ring_kernel,
        name="ring",
        out_shape=(piece,) * 6
        + (jax.ShapeDtypeStruct((rows, ff), BF16),)
        + (jax.ShapeDtypeStruct((width, ff), BF16),) * 2,
        in_specs=[ANY] * 7,
        out_specs=(ANY,) * 9,
        scratch_shapes=[
            pltpu.VMEM((width, ff), BF16),
            pltpu.VMEM((width, ff), BF16),
            pltpu.VMEM((ff, width), BF16),
            pltpu.VMEM((rows, ff), BF16),
            pltpu.VMEM((rows, ff), BF16),
            pltpu.VMEM((2, BLK, width), BF16),
            pltpu.VMEM((2, BLK, ff), BF16),
            pltpu.VMEM((2, BLK, ff), BF16),
            pltpu.VMEM((2, BLK, ff), BF16),
            pltpu.VMEM((12, BLK, half), BF16),
            pltpu.VMEM((12, BLK, half), BF16),
            pltpu.VMEM((2, chunk, half), BF16),
            pltpu.VMEM((2, rows, XT), BF16),
            pltpu.VMEM((2, XT, ff), BF16),
            pltpu.VMEM((2, XT, ff), BF16),
            dma((ff // NT,)),
            dma((2, width // DT)),
            dma((2, 3)),
            dma((2,)),
            dma((12,)),
            dma((12,)),
            dma((2, half // DT)),
            dma((2, half // DT)),
            dma((8,)),
            dma((8,)),
            dma((2, 2)),
            dma((2,)),
            dma((2, 2)),
        ],
        compiler_params=pltpu.CompilerParams(collective_id=0, has_side_effects=True, vmem_limit_bytes=60 << 20),
        cost_estimate=pl.CostEstimate(flops=10 * rows * width * ff, bytes_accessed=100 << 20, transcendentals=rows * ff),
    )(x, dy, gate, up, w_gate, w_up, w_down)


def place_copies(pairs, stage, sems):
    return [
        (pltpu.make_async_copy(s, v, sems.at[i, 0]), pltpu.make_async_copy(v, d, sems.at[i, 1]))
        for i, ((s, d), v) in enumerate(zip(pairs, stage))
    ]


def rest_kernel(hid, dy, own_a, own_b, r_a, r_b, l_a, l_b, g_in, u_in, dw_down, dx, g_out, u_out, pieces, gu, sems):
    me = lax.axis_index("tp")
    chunk, half = own_a.shape
    step, last = pl.program_id(0), pl.num_programs(0) - 1
    pairs, stage = [(g_in, g_out), (u_in, u_out)], [gu.at[0], gu.at[1]]
    for k, (a, b) in ((0, (own_a, own_b)), (1, (r_a, r_b)), (3, (l_a, l_b))):
        r = pl.ds(pl.multiple_of(lax.rem(me + k, 4) * chunk, chunk), chunk)
        for h, src in enumerate((a, b)):
            stage.append(pieces.at[len(pairs) - 2])
            pairs.append((src, dx.at[r, pl.ds(h * half, half)]))
    copies = place_copies(pairs, stage, sems)

    @pl.when(step == 0)
    def _():
        for read, _ in copies:
            read.start()

    dw_down[...] = dot(hid[...], dy[...], 0, 0).astype(BF16)

    @pl.when(step == 1)
    def _():
        for read, write in copies:
            read.wait()
            write.start()

    @pl.when(step == last)
    def _():
        for _, write in copies:
            write.wait()


def rest(hid, dy, pieces, dw_gate, dw_up):
    rows, width = dy.shape
    ff = hid.shape[1]
    chunk, half = rows // 4, width // 2
    return pl.pallas_call(
        rest_kernel,
        name="rest",
        grid=(ff // NT,),
        out_shape=(
            jax.ShapeDtypeStruct((ff, width), BF16),
            jax.ShapeDtypeStruct((rows, width), BF16),
            jax.ShapeDtypeStruct(dw_gate.shape, BF16),
            jax.ShapeDtypeStruct(dw_up.shape, BF16),
        ),
        in_specs=[pl.BlockSpec((rows, NT), lambda i: (0, i)), pl.BlockSpec((rows, width), lambda i: (0, 0))] + [ANY] * 8,
        out_specs=(pl.BlockSpec((NT, width), lambda i: (i, 0)), ANY, ANY, ANY),
        scratch_shapes=[
            pltpu.VMEM((6, chunk, half), BF16),
            pltpu.VMEM((2,) + dw_gate.shape, BF16),
            pltpu.SemaphoreType.DMA((8, 2)),
        ],
        compiler_params=pltpu.CompilerParams(vmem_limit_bytes=56 << 20),
        cost_estimate=pl.CostEstimate(flops=2 * rows * width * ff, bytes_accessed=60 << 20, transcendentals=0),
    )(hid, dy, *pieces, dw_gate, dw_up)


def place_kernel(p_a, p_b, dx_in, dx, stage, sems):
    me = lax.axis_index("tp")
    chunk, half = p_a.shape
    r = pl.ds(pl.multiple_of(lax.rem(me + 2, 4) * chunk, chunk), chunk)
    pairs = [(src, dx.at[r, pl.ds(h * half, half)]) for h, src in enumerate((p_a, p_b))]
    copies = place_copies(pairs, [stage.at[0], stage.at[1]], sems)
    for read, _ in copies:
        read.start()
    for read, write in copies:
        read.wait()
        write.start()
    for _, write in copies:
        write.wait()


def place(p_a, p_b, dx):
    return pl.pallas_call(
        place_kernel,
        name="place",
        out_shape=jax.ShapeDtypeStruct(dx.shape, dx.dtype),
        in_specs=[ANY] * 3,
        out_specs=ANY,
        scratch_shapes=[pltpu.VMEM((2,) + p_a.shape, BF16), pltpu.SemaphoreType.DMA((2, 2))],
        input_output_aliases={2: 0},
        compiler_params=pltpu.CompilerParams(vmem_limit_bytes=8 << 20),
    )(p_a, p_b, dx)


def solution(mesh):
    n = mesh.shape["tp"]
    assert n == 4
    to_left = [(i, (i - 1) % n) for i in range(n)]
    to_right = [(i, (i + 1) % n) for i in range(n)]

    def step(x, dy, gate, up, w_gate, w_up, w_down):
        *pieces, hid, dw_gate, dw_up = ring(x, dy, gate, up, w_gate, w_up, w_down)
        p_a = lax.ppermute(pieces[2], "tp", to_left)
        p_b = lax.ppermute(pieces[5], "tp", to_right)
        dw_down, dx, dw_gate, dw_up = rest(hid, dy, pieces, dw_gate, dw_up)
        return place(p_a, p_b, dx), dw_gate, dw_up, dw_down

    tokens, columns, rows = P("dp", None), P(None, "tp"), P("tp", None)
    return jax.shard_map(
        step,
        mesh=mesh,
        in_specs=(tokens, tokens, P("dp", "tp"), P("dp", "tp"), columns, columns, rows),
        out_specs=(tokens, P("dp", "tp"), P("dp", "tp"), P(("dp", "tp"), None)),
        check_vma=False,
    )
```

```python
import functools
import math

import jax
import jax.numpy as jnp
from jax import lax
from jax.experimental import pallas as pl
from jax.experimental.pallas import tpu as pltpu
from jax.sharding import PartitionSpec as P

MESH = pl.DeviceIdType.MESH
ANY = pl.BlockSpec(memory_space=pl.ANY)
BF16, F32 = jnp.bfloat16, jnp.float32
C = math.sqrt(2.0 / math.pi)
BLK = 256
NT = 256
DT = 512
LATE = 6500
PARTS = 4
DEPTH = 18
RING_VMEM, REST_VMEM = 60, 56
QUICK = (1, 2)
AHEAD = 3
XT = 256

ORDER = ((2, 0), (2, 1), (3, 0), (1, 0), (3, 1), (1, 1), (0, 0), (0, 1))


def dot(a, b, ca, cb):
    return lax.dot_general(a, b, (((ca,), (cb,)), ((), ())), preferred_element_type=F32)


def ring_kernel(
    x, dy, gate, up, w_gate, w_up, w_down,
    own_a, own_b, r_a, r_b, l_a, l_b, hid, dw_gate, dw_up, dw_down,
    wg, wu, wd, dg, du, dyb, gb, ub, hidb, snd, rcv, own, xb, og, ou,
    wd_sem, w_sem, blk_sem, hid_sem, ssem, rsem, part_sem, head_ssem, head_rsem, ag_ssem, ag_rsem, own_sem, x_sem, o_sem, dy_sem,
):
    me = lax.axis_index("tp")
    right, left = lax.rem(me + 1, 4), lax.rem(me + 3, 4)
    rows, width = dy.shape
    ff = gate.shape[1]
    chunk, half = rows // 4, width // 2

    def start_row(j):
        k, b = ORDER[j]
        return pl.multiple_of(lax.rem(me + k, 4) * chunk + b * BLK, BLK)

    def block_copies(j):
        s, r = j % 2, pl.ds(start_row(j), BLK)
        return [
            pltpu.make_async_copy(dy.at[r], dyb.at[s], blk_sem.at[s, 0]),
            pltpu.make_async_copy(gate.at[r], gb.at[s], blk_sem.at[s, 1]),
            pltpu.make_async_copy(up.at[r], ub.at[s], blk_sem.at[s, 2]),
        ]

    def span(n, size):
        return pl.ds(n * size if isinstance(n, int) else pl.multiple_of(n * size, size), size)

    def wd_copy(n):
        r = span(n, NT)
        return pltpu.make_async_copy(w_down.at[r], wd.at[r], wd_sem.at[n])

    def w_copies(q):
        r = span(q, DT)
        return (
            pltpu.make_async_copy(w_gate.at[r], wg.at[r], w_sem.at[0, q]),
            pltpu.make_async_copy(w_up.at[r], wu.at[r], w_sem.at[1, q]),
        )

    def start(copies):
        for c in copies:
            c.start()

    nt, per_half = ff // NT, half // DT
    r0 = pl.ds(start_row(0), BLK)
    parts = [
        [pltpu.make_async_copy(a.at[r0, c], b.at[0, :, c], part_sem.at[i, k]) for i, (a, b) in enumerate(((gate, gb), (up, ub)))]
        for k, c in enumerate((pl.ds(0, NT), pl.ds(NT, ff - NT)))
    ]
    first = pltpu.make_async_copy(dy.at[r0], dyb.at[0], blk_sem.at[0, 0])
    start(parts[0] + [first, wd_copy(0)])

    barrier = pltpu.get_barrier_semaphore()
    for d in (left, right):
        pl.semaphore_signal(barrier, inc=1, device_id={"tp": d}, device_id_type=MESH)

    def hid_copy(j):
        return pltpu.make_async_copy(hidb.at[j % 2], hid.at[pl.ds(start_row(j), BLK)], hid_sem.at[j % 2])

    def backward(j, n, dh):
        s, r, cols = j % 2, pl.ds(start_row(j), BLK), pl.ds(0, ff) if n is None else span(n, NT)
        g = gb[s, :, cols].astype(F32)
        u = ub[s, :, cols].astype(F32)
        g2 = g * g
        t = jnp.tanh(C * (g + 0.044715 * (g * g2)))
        cdf = 0.5 * (1.0 + t)
        act = g * cdf
        hidb[s, :, cols] = (act * u).astype(BF16)
        du[r, cols] = (dh * act).astype(BF16)
        slope = cdf + (0.5 * C) * g * (1.0 - t * t) * (1.0 + (3 * 0.044715) * g2)
        dg[r, cols] = (dh * u * slope).astype(BF16)

    def hidden_first():
        for c in parts[0]:
            c.wait()
        start([wd_copy(n) for n in range(1, AHEAD)] + parts[1])
        first.wait()

        @pl.loop(0, nt)
        def _(n):
            wd_copy(n).wait()

            @pl.when(n == 1)
            def _():
                for c in parts[1]:
                    c.wait()

            @pl.when(n < nt - AHEAD)
            def _():
                wd_copy(n + AHEAD).start()

            @pl.when(n >= nt - AHEAD)
            def _():
                i = n - (nt - AHEAD)
                start(w_copies(lax.rem(i, 2) * per_half + i // 2))

            backward(0, n, dot(dyb[0], wd[span(n, NT), :], 1, 1))

        for i in range(AHEAD, 2 * per_half):
            start(w_copies(i % 2 * per_half + i // 2))
        start(block_copies(1))
        hid_copy(0).start()

    def hidden(j):
        s = j % 2
        for c in block_copies(j):
            c.wait()
        if j >= 2:
            hid_copy(j - 2).wait()

        if j in QUICK:
            backward(j, None, dot(dyb[s], wd[...], 1, 1))
        else:

            @pl.loop(0, nt)
            def _(n):
                backward(j, n, dot(dyb[s], wd[span(n, NT), :], 1, 1))

        if j < len(ORDER) - 2:
            for c in block_copies(j + 2):
                c.start()
        hid_copy(j).start()

    def columns(j, wr, adds, dst, rows_, cols):
        r = pl.ds(start_row(j), BLK)
        t = dot(dg[r, :], wg[wr, :], 1, 1) + dot(du[r, :], wu[wr, :], 1, 1)
        for a in adds:
            t = t + rcv[a, :, cols].astype(F32)
        dst[rows_, cols] = t.astype(BF16)

    def term(j, h, adds, dst, row):
        if j in QUICK:
            columns(j, pl.ds(h * half, half), adds, dst, pl.ds(row, BLK), pl.ds(0, half))
            return

        @pl.loop(0, per_half)
        def _(i):
            columns(j, span(h * per_half + i, DT), adds, dst, pl.ds(row, BLK), span(i, DT))

    def slot(kind, b):
        return kind * 2 + b

    def reduce_copy(kind, b, rect=None):
        s = slot(kind, b)
        src, dst, sems = snd.at[s], rcv.at[s], (ssem.at[s], rsem.at[s])
        if rect is not None:
            src, dst = src.at[:, span(rect, DT)], dst.at[:, span(rect, DT)]
            sems = (head_ssem.at[kind // 3, rect], head_rsem.at[kind // 3, rect])
        return pltpu.make_async_remote_copy(
            src_ref=src, dst_ref=dst, send_sem=sems[0], recv_sem=sems[1],
            device_id={"tp": left if kind < 3 else right}, device_id_type=MESH,
        )

    def send(j, h, kind, adds=()):
        b = ORDER[j][1]
        term(j, h, adds, snd.at[slot(kind, b)], 0)
        reduce_copy(kind, b).start()

    heads = half // DT
    head = range(heads)
    hidden_first()
    pl.semaphore_wait(barrier, 2)

    @pl.when(lax.rem(lax.axis_index("dp"), 2) == 0)
    def _():
        pl.delay(LATE)

    @pl.loop(0, heads)
    def _(i):
        for h, kind in ((0, 0), (1, 3)):
            for c in w_copies(h * per_half + i):
                c.wait()
            columns(0, span(h * heads + i, DT), (), snd.at[slot(kind, 0)], pl.ds(0, BLK), span(i, DT))
            reduce_copy(kind, 0, i).start()

    start(block_copies(2))
    hidden(1)
    send(1, 0, 0)
    send(1, 1, 3)
    for j, h, kind in ((2, 1, 1), (3, 0, 4), (4, 1, 1), (5, 0, 4)):
        hidden(j)
        send(j, h, kind)
    for b in range(2):
        for kind, j, h in ((0, 2, 0), (3, 3, 1)):
            for i in head if b == 0 else (None,):
                reduce_copy(kind, b, i).wait_recv()
            send(j + 2 * b, h, kind + 2, (slot(kind, b),))
    hidden(6)
    hidden(7)

    steps = width // XT

    def x_copy(i, s):
        return pltpu.make_async_copy(x.at[:, pl.ds(pl.multiple_of(i * XT, XT), XT)], xb.at[s], x_sem.at[s])

    def o_copies(i, s):
        r = pl.ds(pl.multiple_of(i * XT, XT), XT)
        return (
            pltpu.make_async_copy(og.at[s], dw_gate.at[r], o_sem.at[s, 0]),
            pltpu.make_async_copy(ou.at[s], dw_up.at[r], o_sem.at[s, 1]),
        )

    def weights(lo, hi):
        x_copy(lo, 0).start()
        x_copy(lo + 1, 1).start()

        @pl.loop(0, (hi - lo) // 2)
        def _(p):
            for s in range(2):
                i = lo + 2 * p + s
                x_copy(i, s).wait()

                @pl.when(p > 0)
                def _():
                    for c in o_copies(i, s):
                        c.wait()

                og[s] = dot(xb[s], dg[...], 0, 0).astype(BF16)
                ou[s] = dot(xb[s], du[...], 0, 0).astype(BF16)

                @pl.when(i + 2 < hi)
                def _():
                    x_copy(i + 2, s).start()

                for c in o_copies(i, s):
                    c.start()

        for s in range(2):
            for c in o_copies(hi - 2 + s, s):
                c.wait()

    dy_halves = (wg.at[:, pl.ds(0, half)], wu.at[:, pl.ds(0, half)])
    dy_copies = [pltpu.make_async_copy(dy.at[:, pl.ds(h * half, half)], v, dy_sem.at[h]) for h, v in enumerate(dy_halves)]

    def down():
        def load(i, s):
            return pltpu.make_async_copy(hid.at[:, span(i, XT)], xb.at[s], x_sem.at[s])

        def save(i, s):
            r = span(i, XT)
            return (
                pltpu.make_async_copy(og.at[s, :, pl.ds(0, half)], dw_down.at[r, pl.ds(0, half)], o_sem.at[s, 0]),
                pltpu.make_async_copy(ou.at[s, :, pl.ds(0, half)], dw_down.at[r, pl.ds(half, half)], o_sem.at[s, 1]),
            )

        load(0, 0).start()
        load(1, 1).start()
        for c in dy_copies:
            c.wait()

        @pl.loop(0, nt)
        def _(i):
            s = lax.rem(i, 2)
            load(i, s).wait()

            @pl.when(i >= 2)
            def _():
                for c in save(i, s):
                    c.wait()

            og[s, :, :half] = dot(xb[s], wg[:, :half], 0, 0).astype(BF16)
            ou[s, :, :half] = dot(xb[s], wu[:, :half], 0, 0).astype(BF16)

            @pl.when(i + 2 < nt)
            def _():
                load(i + 2, s).start()

            start(save(i, s))

        for i in (nt - 2, nt - 1):
            for c in save(i, i % 2):
                c.wait()

    def gather_copies(b):
        r = pl.ds(b * BLK, BLK)
        for d, h, dst in ((left, 0, r_a), (right, 1, l_b), (left, 1, r_b), (right, 0, l_a)):
            i = b * 4 + (0 if d is left else 2) + h
            yield pltpu.make_async_remote_copy(
                src_ref=own.at[h, r], dst_ref=dst.at[r], send_sem=ag_ssem.at[i], recv_sem=ag_rsem.at[i],
                device_id={"tp": d}, device_id_type=MESH,
            )

    def own_copies(b):
        r = pl.ds(b * BLK, BLK)
        return (
            pltpu.make_async_copy(own.at[0, r], own_a.at[r], own_sem.at[b, 0]),
            pltpu.make_async_copy(own.at[1, r], own_b.at[r], own_sem.at[b, 1]),
        )

    def finish(b):
        reduce_copy(4, b).wait_recv()
        reduce_copy(2, b).wait_recv()
        term(6 + b, 0, (slot(2, b), slot(4, b)), own.at[0], b * BLK)
        reduce_copy(1, b).wait_recv()
        reduce_copy(5, b).wait_recv()
        term(6 + b, 1, (slot(5, b), slot(1, b)), own.at[1], b * BLK)
        for c in gather_copies(b):
            c.start()
        for c in own_copies(b):
            c.start()

    weights(0, steps // 2)
    finish(0)
    finish(1)
    start(dy_copies)
    hid_copy(6).wait()
    hid_copy(7).wait()
    weights(steps // 2, steps)
    down()

    for kind in range(6):
        for b in range(2):
            for i in head if kind % 3 == 0 and b == 0 else (None,):
                reduce_copy(kind, b, i).wait_send()
    for b in range(2):
        for c in gather_copies(b):
            c.wait()
        for c in own_copies(b):
            c.wait()


def ring(x, dy, gate, up, w_gate, w_up, w_down):
    rows, width = dy.shape
    ff = gate.shape[1]
    chunk, half = rows // 4, width // 2
    assert rows == width and half <= ff
    piece = jax.ShapeDtypeStruct((chunk, half), BF16)
    dma = pltpu.SemaphoreType.DMA
    return pl.pallas_call(
        ring_kernel,
        name="ring",
        out_shape=(piece,) * 6
        + (jax.ShapeDtypeStruct((rows, ff), BF16),)
        + (jax.ShapeDtypeStruct((width, ff), BF16),) * 2
        + (jax.ShapeDtypeStruct((ff, width), BF16),),
        in_specs=[ANY] * 7,
        out_specs=(ANY,) * 10,
        scratch_shapes=[
            pltpu.VMEM((width, ff), BF16),
            pltpu.VMEM((width, ff), BF16),
            pltpu.VMEM((ff, width), BF16),
            pltpu.VMEM((rows, ff), BF16),
            pltpu.VMEM((rows, ff), BF16),
            pltpu.VMEM((2, BLK, width), BF16),
            pltpu.VMEM((2, BLK, ff), BF16),
            pltpu.VMEM((2, BLK, ff), BF16),
            pltpu.VMEM((2, BLK, ff), BF16),
            pltpu.VMEM((12, BLK, half), BF16),
            pltpu.VMEM((12, BLK, half), BF16),
            pltpu.VMEM((2, chunk, half), BF16),
            pltpu.VMEM((2, rows, XT), BF16),
            pltpu.VMEM((2, XT, ff), BF16),
            pltpu.VMEM((2, XT, ff), BF16),
            dma((ff // NT,)),
            dma((2, width // DT)),
            dma((2, 3)),
            dma((2,)),
            dma((12,)),
            dma((12,)),
            dma((2, 2)),
            dma((2, half // DT)),
            dma((2, half // DT)),
            dma((8,)),
            dma((8,)),
            dma((2, 2)),
            dma((2,)),
            dma((2, 2)),
            dma((2,)),
        ],
        compiler_params=pltpu.CompilerParams(collective_id=0, has_side_effects=True, vmem_limit_bytes=RING_VMEM << 20),
        cost_estimate=pl.CostEstimate(flops=12 * rows * width * ff, bytes_accessed=100 << 20, transcendentals=rows * ff),
    )(x, dy, gate, up, w_gate, w_up, w_down)


def place_copies(pairs, stage, sems):
    return [
        (pltpu.make_async_copy(s, v, sems.at[i, 0]), pltpu.make_async_copy(v, d, sems.at[i, 1]))
        for i, ((s, d), v) in enumerate(zip(pairs, stage))
    ]


def rest_kernel(own_a, own_b, r_a, r_b, l_a, l_b, g_in, u_in, d_in, dx, g_out, u_out, d_out, pieces, gu, dn, sems):
    me = lax.axis_index("tp")
    chunk, half = own_a.shape
    pairs, stage = [], []
    for k, (a, b) in ((0, (own_a, own_b)), (1, (r_a, r_b)), (3, (l_a, l_b))):
        r = pl.ds(pl.multiple_of(lax.rem(me + k, 4) * chunk, chunk), chunk)
        for h, src in enumerate((a, b)):
            stage.append(pieces.at[len(pairs)])
            pairs.append((src, dx.at[r, pl.ds(h * half, half)]))
    for src, dst, v in ((g_in, g_out, gu.at[0]), (u_in, u_out, gu.at[1]), (d_in, d_out, dn)):
        n = src.shape[0] // PARTS
        for i in range(PARTS):
            r = pl.ds(i * n, n)
            pairs.append((src.at[r], dst.at[r]))
            stage.append(v.at[r])
    copies = place_copies(pairs, stage, sems)
    for read, _ in copies[:DEPTH]:
        read.start()
    for i, (read, write) in enumerate(copies):
        read.wait()
        write.start()
        if i + DEPTH < len(copies):
            copies[i + DEPTH][0].start()
    for _, write in copies:
        write.wait()


def rest(pieces, dw_gate, dw_up, dw_down):
    chunk, half = pieces[0].shape
    grads = (dw_gate, dw_up, dw_down)
    dx = jax.ShapeDtypeStruct((4 * chunk, 2 * half), BF16)
    moved = 6 * pieces[0].size + 3 * dw_gate.size
    return pl.pallas_call(
        rest_kernel,
        name="rest",
        out_shape=(dx, *(jax.ShapeDtypeStruct(g.shape, BF16) for g in grads)),
        in_specs=[ANY] * 9,
        out_specs=(ANY,) * 4,
        scratch_shapes=[
            pltpu.VMEM((6, chunk, half), BF16),
            pltpu.VMEM((2,) + dw_gate.shape, BF16),
            pltpu.VMEM(dw_down.shape, BF16),
            pltpu.SemaphoreType.DMA((6 + 3 * PARTS, 2)),
        ],
        compiler_params=pltpu.CompilerParams(vmem_limit_bytes=REST_VMEM << 20),
        cost_estimate=pl.CostEstimate(flops=12_000_000_000, bytes_accessed=4 * moved, transcendentals=0),
    )(*pieces, *grads)


def place_kernel(p_a, p_b, dx_in, dx, stage, sems):
    me = lax.axis_index("tp")
    chunk, half = p_a.shape
    r = pl.ds(pl.multiple_of(lax.rem(me + 2, 4) * chunk, chunk), chunk)
    pairs = [(src, dx.at[r, pl.ds(h * half, half)]) for h, src in enumerate((p_a, p_b))]
    copies = place_copies(pairs, [stage.at[0], stage.at[1]], sems)
    for read, _ in copies:
        read.start()
    for read, write in copies:
        read.wait()
        write.start()
    for _, write in copies:
        write.wait()


def place(p_a, p_b, dx):
    return pl.pallas_call(
        place_kernel,
        name="place",
        out_shape=jax.ShapeDtypeStruct(dx.shape, dx.dtype),
        in_specs=[ANY] * 3,
        out_specs=ANY,
        scratch_shapes=[pltpu.VMEM((2,) + p_a.shape, BF16), pltpu.SemaphoreType.DMA((2, 2))],
        input_output_aliases={2: 0},
        compiler_params=pltpu.CompilerParams(vmem_limit_bytes=8 << 20),
    )(p_a, p_b, dx)


def solution(mesh):
    n = mesh.shape["tp"]
    assert n == 4
    to_left = [(i, (i - 1) % n) for i in range(n)]
    to_right = [(i, (i + 1) % n) for i in range(n)]

    def step(x, dy, gate, up, w_gate, w_up, w_down):
        *pieces, _, dw_gate, dw_up, dw_down = ring(x, dy, gate, up, w_gate, w_up, w_down)
        p_a = lax.ppermute(pieces[2], "tp", to_left)
        p_b = lax.ppermute(pieces[5], "tp", to_right)
        dx, *grads = rest(pieces, dw_gate, dw_up, dw_down)
        return place(p_a, p_b, dx), *grads

    tokens, columns, rows = P("dp", None), P(None, "tp"), P("tp", None)
    return jax.shard_map(
        step,
        mesh=mesh,
        in_specs=(tokens, tokens, P("dp", "tp"), P("dp", "tp"), columns, columns, rows),
        out_specs=(tokens, P("dp", "tp"), P("dp", "tp"), P(("dp", "tp"), None)),
        check_vma=False,
    )
```
